256 devices in a mesh: row: 16 (over y, z_hi, core), col: 16 (over z_lo, x).
Axes of the slice: x: 4, y: 4, z: 8 (z_hi: 2, z_lo: 4; z = z_hi * 4 + z_lo), core: 2. Of those that a mesh axis runs over, the one named last changes fastest.
Arguments:
- fluid_data: float32 [51, 32768], P(None, ('row', 'col')), as said below
- center_data: float32 [51, 16384], P(None, ('col', 'row')), as said below
- poly_coef: float32 [48, 4], replicated, may hold values from -3 to 3
Outputs:
- fluid_motion: float32 [48, 32768], P(None, ('row', 'col'))
- center_load: float32 [48, 16384], P(None, ('col', 'row'))
The draws below stay inside these ranges and needn't reach their ends.
Inputs may be any that keep to these rules, and one draw needn't show every extreme that they name: Rows 0 to 2 of fluid_data lie in [0, 1]; rows 3 and on are forces. Rows 0 and 1 of center_data lie in [0, 1] and row 2 lies in [-0.5, -0.02], so every center is at least 0.02 below every vertex; rows 3 and on are coefficients.
All inputs are finite; a program needn't handle non-finite values.
Results may differ from the reference program's by a relative error of at most 0.0003.
Values sent between devices are 32-bit elements; how exact they have to be, the bound alone decides.
A program may use at most 64 MiB of HBM per device.

```python
import math
import jax
import jax.numpy as jnp
from jax import lax

WAVES = 64
COLS = 48
FLUID = 32768
CENTERS = 16384


def draw_fluid_data(key, part):
    first, second = jax.random.split(jax.random.fold_in(key, 11))
    places = jax.random.uniform(first, (3, FLUID), jnp.float32)
    spread = 2.0 * math.pi * WAVES * math.sqrt(0.8 / FLUID)
    values = jax.random.normal(second, (COLS, FLUID), jnp.float32) * spread
    return jnp.concatenate([places, values], axis=0)


def draw_center_data(key, part):
    first, second, third = jax.random.split(jax.random.fold_in(key, 23), 3)
    plane = jax.random.uniform(first, (2, CENTERS), jnp.float32)
    depth = jax.random.uniform(second, (1, CENTERS), jnp.float32)
    spread = 2.0 * math.pi * WAVES * math.sqrt(0.8 / CENTERS)
    height = -0.02 - 0.48 * depth
    values = jax.random.normal(third, (COLS, CENTERS), jnp.float32) * spread
    return jnp.concatenate([plane, height, values], axis=0)


def noise(key, dims, scale, limit, kind=jnp.bfloat16):
    entries = scale * jax.random.normal(key, dims, jnp.float32)
    return jnp.clip(entries, min=-limit, max=limit).astype(kind)


def setup_inputs(seed: int = 0) -> dict:
    streams_of = jax.random.split(jax.random.key(seed), 4)
    fluid_data = draw_fluid_data(jax.random.fold_in(streams_of[3], 71), 0)
    center_data = draw_center_data(jax.random.fold_in(streams_of[3], 71), 0)
    poly_coef = noise(streams_of[2], (COLS, 4), 0.5, 3.0, jnp.float32)
    return dict(fluid_data=fluid_data, center_data=center_data, poly_coef=poly_coef)


def kernel_block(center_pos, fluid_pos):
    dx = center_pos[0][:, None] - fluid_pos[0][None, :]
    dy = center_pos[1][:, None] - fluid_pos[1][None, :]
    dz = center_pos[2][:, None] - fluid_pos[2][None, :]
    sq = dx * dx + dy * dy + dz * dz
    phase = 2.0 * math.pi * WAVES * jnp.sqrt(sq)
    return jnp.sin(phase) / phase

def reference(fluid_data, center_data, poly_coef):
    total = center_data.shape[1]
    width = fluid_data.shape[1]
    block = math.gcd(total, 256)
    count = total // block
    fluid_pos = fluid_data[:3]
    forces = fluid_data[3:]
    pieces = center_data.reshape(center_data.shape[0], count, block).transpose(1, 0, 2)

    def step(motion, piece):
        tile = kernel_block(piece[:3], fluid_pos)
        motion = motion + jnp.dot(piece[3:], tile, precision=lax.Precision.HIGHEST, preferred_element_type=jnp.float32)
        back = lax.dot_general(forces, tile, (((1,), (1,)), ((), ())), precision=lax.Precision.HIGHEST, preferred_element_type=jnp.float32)
        return (motion, back)
    start = jnp.zeros((forces.shape[0], width), jnp.float32)
    motion, backs = lax.scan(step, start, pieces)
    loads = backs.transpose(1, 0, 2).reshape(forces.shape[0], total)
    affine = poly_coef[:, 0:1] + jnp.dot(poly_coef[:, 1:], fluid_pos, precision=lax.Precision.HIGHEST, preferred_element_type=jnp.float32)
    return (motion + affine, loads)
```

```python
import jax
import jax.numpy as jnp
from jax import lax
from jax.experimental import pallas as pl
from jax.experimental.pallas import tpu as pltpu
from jax.sharding import PartitionSpec as P

WAVES = 64
COLS = 48
PLANE = [
    (0, 0), (1, 0), (3, 0), (0, 1), (0, 3), (2, 0), (0, 2), (1, 1),
    (1, 3), (3, 1), (3, 3), (2, 1), (2, 3), (1, 2), (3, 2), (2, 2),
]
LINE = [
    (0, 0), (0, 1), (1, 0), (1, 1), (7, 0), (7, 1), (2, 0), (2, 1),
    (6, 0), (6, 1), (3, 0), (3, 1), (5, 0), (5, 1), (4, 0), (4, 1),
]
HALF = 512
TILES = 8
STRIP = 32
S = (0.9999999765898422, -6.57972875383963, 12.987203158835507, -12.183276227896942, 6.292462070004323)
F32 = jnp.float32
BF16 = jnp.bfloat16


def split(value):
    high = value.astype(BF16)
    return high, (value - high.astype(F32)).astype(BF16)


def body(
    fluid_ref, center_ref, poly_ref, motion_ref, load_ref,
    fbuf, cbuf, cb, fpos, fhl, chl, kh0, kl0, kh1, kl1, lacc, macc, mrecv, lsend, lrecv,
    fs, fr, cs, cr, ms, mr, ls, lr,
):
    row, col = lax.axis_index("row"), lax.axis_index("col")
    core, z_hi, y = row % 2, (row // 2) % 2, row // 4
    x, z_lo = col % 4, col // 4
    z = z_hi * 4 + z_lo

    def plane_dev(k):
        dx, dy = PLANE[k]
        return {"row": (row + 4 * dy) % 16, "col": z_lo * 4 + (x + dx) % 4}

    def line_dev(k):
        dz, dc = LINE[k]
        z2 = (z + dz) % 8
        return {"row": 4 * y + 2 * (z2 // 4) + (core + dc) % 2, "col": (z2 % 4) * 4 + x}

    def back_plane_dev(k):
        dx, dy = PLANE[k]
        return {"row": (row + 4 * (4 - dy)) % 16, "col": z_lo * 4 + (x + 4 - dx) % 4}

    def back_line_dev(k):
        dz, dc = LINE[k]
        z2 = (z + 8 - dz) % 8
        return {"row": 4 * y + 2 * (z2 // 4) + (core + dc) % 2, "col": (z2 % 4) * 4 + x}

    def remote(src, dst, send, recv, dev):
        return pltpu.make_async_remote_copy(
            src_ref=src, dst_ref=dst, send_sem=send, recv_sem=recv,
            device_id=dev, device_id_type=pl.DeviceIdType.MESH,
        )

    barrier = pltpu.get_barrier_semaphore()
    for k in range(1, 16):
        for dev in (plane_dev(k), line_dev(k)):
            pl.semaphore_signal(barrier, inc=1, device_id=dev, device_id_type=pl.DeviceIdType.MESH)

    fbuf[0, 0:COLS, :] = fluid_ref[3:51, :]
    fbuf[0, COLS:56, :] = jnp.zeros((8, 128), F32)
    fbuf[0, COLS:51, :] = fluid_ref[0:3, :] * WAVES
    cbuf[0, 0:24, 0:64] = center_ref[3:27, :]
    cbuf[0, 0:24, 64:128] = center_ref[27:51, :]
    cbuf[0, 24:32, :] = jnp.zeros((8, 128), F32)
    cbuf[0, 24:27, 0:64] = center_ref[0:3, :] * WAVES
    fhl[:, 96:128, :] = jnp.zeros((TILES, 32, 256), BF16)

    pl.semaphore_wait(barrier, 30)
    fcopy = [None] + [
        remote(fbuf.at[0], fbuf.at[k], fs.at[k], fr.at[k], plane_dev(k)) for k in range(1, 16)
    ]
    ccopy = [None] + [
        remote(cbuf.at[0], cbuf.at[k], cs.at[k], cr.at[k], line_dev(k)) for k in range(1, 16)
    ]
    for k in range(1, 16):
        ccopy[k].start()
        fcopy[k].start()

    low = lax.broadcasted_iota(jnp.int32, (24, 128), 1) < 64

    def turn(value):
        return pltpu.roll(value, 64, 1)

    def unpack_centers(m):
        a, b = cbuf[2 * m], cbuf[2 * m + 1]
        lanes = pl.ds(m * 128, 128)
        coef = jnp.concatenate(
            [jnp.where(low, a[0:24], turn(b[0:24])), jnp.where(low, turn(a[0:24]), b[0:24])], axis=0
        )
        high, rest = split(coef)
        chl[0:COLS, lanes] = high
        chl[COLS:96, lanes] = rest
        places = jnp.where(low[0:8], a[24:32], turn(b[24:32]))
        for axis in range(3):
            line = jnp.broadcast_to(places[axis : axis + 1], (128, 128))
            cb[axis, m * 128 : (m + 1) * 128, :] = line.T

    def unpack_fluid(n):
        for part in range(2):
            high, rest = split(fbuf[2 * n + part, 0:COLS, :])
            lanes = pl.ds(part * 128, 128)
            fhl[n, 0:COLS, lanes] = high
            fhl[n, COLS:96, lanes] = rest

    def kernel_tile(half, n, kh, kl):
        places = [[fbuf[2 * n + part, COLS + axis : COLS + axis + 1, :] for axis in range(3)] for part in range(2)]
        for first in range(0, HALF, STRIP):
            rows = pl.ds(half * HALF + first, STRIP)
            at = [cb[axis, rows, :] for axis in range(3)]
            for part in range(2):
                dx, dy, dz = (at[axis] - places[part][axis] for axis in range(3))
                sq = dx * dx + dy * dy + dz * dz
                inverse = lax.rsqrt(sq)
                turns = sq * inverse - 0.25
                b = 0.25 - jnp.abs(turns - jnp.round(turns))
                b2 = b * b
                value = S[4]
                for coefficient in (S[3], S[2], S[1], S[0]):
                    value = value * b2 + coefficient
                high, rest = split(value * (b * inverse))
                kh[first : first + STRIP, part * 128 : (part + 1) * 128] = high
                kl[first : first + STRIP, part * 128 : (part + 1) * 128] = rest

    def products(half, n, kh, kl):
        coef = chl[:, half * HALF : (half + 1) * HALF]
        high, rest = kh[...], kl[...]
        motion = jnp.dot(coef, high, preferred_element_type=F32) + jnp.dot(
            coef, rest, preferred_element_type=F32
        )
        motion = motion[0:COLS] + motion[COLS:96]
        for part in range(2):
            piece = motion[:, part * 128 : (part + 1) * 128]
            if half == 0:
                macc[2 * n + part] = piece
            else:
                macc[2 * n + part] += piece
        forces = fhl[n]
        across = (((1,), (1,)), ((), ()))
        load = lax.dot_general(high, forces, across, preferred_element_type=F32) + lax.dot_general(
            rest, forces, across, preferred_element_type=F32
        )
        if n == (0 if half == 0 else TILES - 1):
            lacc[half] = load
        else:
            lacc[half] += load

    def send_loads(half):
        total = lacc[half]
        total = (total + pltpu.roll(total, 80, 1)).T[0:COLS]
        copies = []
        for pair in range(4):
            m = half * 4 + pair
            piece = total[:, pair * 128 : (pair + 1) * 128]
            top, bottom = piece[0:24], piece[24:48]
            lsend[2 * m] = jnp.where(low, top, turn(bottom))
            lsend[2 * m + 1] = jnp.where(low, turn(top), bottom)
            for k in (2 * m, 2 * m + 1):
                if k > 0:
                    copy = remote(lsend.at[k], lrecv.at[k], ls.at[k], lr.at[k], back_line_dev(k))
                    copy.start()
                    copies.append(copy)
        return copies

    def send_motion(n):
        copies = []
        for k in (2 * n, 2 * n + 1):
            if k > 0:
                copy = remote(macc.at[k], mrecv.at[k], ms.at[k], mr.at[k], back_plane_dev(k))
                copy.start()
                copies.append(copy)
        return copies

    buffers = ((kh0, kl0), (kh1, kl1))
    order = [(0, n) for n in range(TILES)] + [(1, n) for n in reversed(range(TILES))]
    sent = []
    for m in range(4):
        for k in (2 * m, 2 * m + 1):
            if k > 0:
                ccopy[k].wait_recv()
        unpack_centers(m)
    for step, (half, n) in enumerate(order):
        if half == 0:
            for k in (2 * n, 2 * n + 1):
                if k > 0:
                    fcopy[k].wait_recv()
            unpack_fluid(n)
        if half == 1 and n == TILES - 1:
            for m in range(4, 8):
                for k in (2 * m, 2 * m + 1):
                    ccopy[k].wait_recv()
                unpack_centers(m)
        kernel_tile(half, n, *buffers[step % 2])
        if step > 0:
            products(*order[step - 1], *buffers[(step - 1) % 2])
        if step > 1 and order[step - 2][0] == 1:
            sent += send_motion(order[step - 2][1])
        if step > 1 and order[step - 2] == (0, TILES - 1):
            sent += send_loads(0)
    products(*order[-1], *buffers[(len(order) - 1) % 2])
    sent += send_motion(order[-2][1])
    sent += send_loads(1)
    sent += send_motion(order[-1][1])

    motion = macc[0] + poly_ref[:, 0:1]
    for axis in range(3):
        motion += poly_ref[:, axis + 1 : axis + 2] * fluid_ref[axis : axis + 1, :]
    for copy in sent:
        copy.wait_recv()
    for k in range(1, 16):
        motion += mrecv[k]
    motion_ref[...] = motion
    load = lsend[0]
    for k in range(1, 16):
        load += lrecv[k]
    load_ref[0:24, :] = load[:, 0:64]
    load_ref[24:48, :] = load[:, 64:128]

    for copy in sent:
        copy.wait_send()
    for k in range(1, 16):
        fcopy[k].wait_send()
        ccopy[k].wait_send()


def per_device(fluid_data, center_data, poly_coef):
    vmem = pl.BlockSpec(memory_space=pltpu.VMEM)
    dma = pltpu.SemaphoreType.DMA((16,))
    return pl.pallas_call(
        body,
        out_shape=(
            jax.ShapeDtypeStruct((COLS, 128), F32),
            jax.ShapeDtypeStruct((COLS, 64), F32),
        ),
        in_specs=[vmem] * 3,
        out_specs=(vmem, vmem),
        scratch_shapes=[
            pltpu.VMEM((16, 56, 128), F32),
            pltpu.VMEM((16, 32, 128), F32),
            pltpu.VMEM((3, 1024, 128), F32),
            pltpu.VMEM((8, 128), F32),
            pltpu.VMEM((TILES, 128, 256), BF16),
            pltpu.VMEM((96, 1024), BF16),
            pltpu.VMEM((HALF, 256), BF16),
            pltpu.VMEM((HALF, 256), BF16),
            pltpu.VMEM((HALF, 256), BF16),
            pltpu.VMEM((HALF, 256), BF16),
            pltpu.VMEM((2, HALF, 128), F32),
            pltpu.VMEM((16, COLS, 128), F32),
            pltpu.VMEM((16, COLS, 128), F32),
            pltpu.VMEM((16, 24, 128), F32),
            pltpu.VMEM((16, 24, 128), F32),
            *([dma] * 8),
        ],
        compiler_params=pltpu.CompilerParams(collective_id=0, has_side_effects=True),
        name="couple",
    )(fluid_data, center_data, poly_coef)


def solution(mesh):
    return jax.shard_map(
        per_device,
        mesh=mesh,
        in_specs=(P(None, ("row", "col")), P(None, ("col", "row")), P()),
        out_specs=(P(None, ("row", "col")), P(None, ("col", "row"))),
        check_vma=False,
    )
```

```python
import jax
import jax.numpy as jnp
from jax import lax
from jax.experimental import pallas as pl
from jax.experimental.pallas import tpu as pltpu
from jax.sharding import PartitionSpec as P

WAVES = 64
COLS = 48
PLANE = [
    (2, 2), (1, 2), (3, 2), (2, 1), (2, 3), (3, 3), (3, 1), (1, 3),
    (0, 0), (1, 0), (3, 0), (0, 1), (0, 3), (2, 0), (0, 2), (1, 1),
]
OWN = 8
OTHERS = [0, 1, 2, 3, 4, 5, 6, 7, 15, 14, 13, 12, 11, 10, 9]
LINE = [0, 1, 7, 2, 6, 3, 5, 4]
PAIRS = [(0, 2), (4, 6), (8, 10), (12, 14), (1, 3), (5, 7), (9, 11), (13, 15)]
FIRST = [0, 1, 2, 3, 4, 5, 6, 7]
SECOND = [7, 6, 5, 3, 4, 2, 1, 0]
HALF = 512
TILES = 8
STRIP = 32
SCALE = 6.292462070004323
S = [s / SCALE for s in (0.9999999765898422, -6.57972875383963, 12.987203158835507, -12.183276227896942)]
F32 = jnp.float32
BF16 = jnp.bfloat16


def split(value):
    high = value.astype(BF16)
    return high, (value - high.astype(F32)).astype(BF16)


def body(
    fluid_hbm, center_hbm, poly_hbm, motion_ref, load_ref,
    fluid_ref, center_ref, poly_ref, fbuf, cbuf, cb, fhl, chl, kh0, kl0, kh1, kl1, lacc, macc, msib, mout, mrecv, lsend, lrecv, own,
    ins, fs, fr, cs, cr, ss, sr, ms, mr, ls, lr,
):
    row, col = lax.axis_index("row"), lax.axis_index("col")
    core, z_hi, y = row % 2, (row // 2) % 2, row // 4
    x, z_lo = col % 4, col // 4
    z = z_hi * 4 + z_lo

    def plane_dev(dx, dy):
        return {"row": (row + 4 * dy) % 16, "col": z_lo * 4 + (x + dx) % 4}

    def line_dev(dz, flip=0):
        z2 = (z + dz) % 8
        return {"row": 4 * y + 2 * (z2 // 4) + (core + flip) % 2, "col": (z2 % 4) * 4 + x}

    def remote(src, dst, send, recv, dev):
        return pltpu.make_async_remote_copy(
            src_ref=src, dst_ref=dst, send_sem=send, recv_sem=recv,
            device_id=dev, device_id_type=pl.DeviceIdType.MESH,
        )

    fetched = [
        pltpu.make_async_copy(source, target, ins.at[i])
        for i, (source, target) in enumerate(
            ((fluid_hbm, fluid_ref), (center_hbm, center_ref), (poly_hbm, poly_ref))
        )
    ]
    for copy in fetched:
        copy.start()
    sibling = line_dev(0, 1)
    barrier = pltpu.get_barrier_semaphore()
    peers = [plane_dev(*PLANE[k]) for k in OTHERS]
    peers += [line_dev(LINE[i]) for i in range(1, 8)] + [sibling]
    for dev in peers:
        pl.semaphore_signal(barrier, inc=1, device_id=dev, device_id_type=pl.DeviceIdType.MESH)

    for copy in fetched:
        copy.wait()

    fbuf[0, 0:COLS, :] = fluid_ref[3:51, :]
    fbuf[0, COLS:51, :] = fluid_ref[0:3, :] * WAVES
    cbuf[OWN, 0:24, 0:64] = center_ref[3:27, :]
    cbuf[OWN, 0:24, 64:128] = center_ref[27:51, :]
    cbuf[OWN, 24:27, :] = jnp.zeros((3, 128), F32)
    cbuf[OWN, 24:27, 0:64] = center_ref[0:3, :] * WAVES
    fhl[:, 96:128, :] = jnp.zeros((TILES, 32, 256), BF16)

    def poly_column(which):
        return jnp.broadcast_to(poly_ref[which : which + 1, :], (128, COLS)).T

    affine = poly_column(0)
    for axis in range(3):
        affine += poly_column(axis + 1) * fluid_ref[axis : axis + 1, :]
    own[...] = affine

    pl.semaphore_wait(barrier, len(peers))
    started = []

    def start(copy):
        copy.start()
        started.append(copy)
        return copy

    ccopy = {
        k: remote(cbuf.at[OWN], cbuf.at[k], cs.at[k], cr.at[k], plane_dev(*PLANE[k])) for k in OTHERS
    }
    fcopy = [None] * 16
    fcopy[1] = remote(fbuf.at[0], fbuf.at[1], fs.at[1], fr.at[1], sibling)
    for i in range(1, 8):
        fcopy[2 * i] = remote(
            fbuf.at[0], fbuf.at[2 * i], fs.at[2 * i], fr.at[2 * i], line_dev(LINE[i])
        )
        fcopy[2 * i + 1] = remote(
            fbuf.at[2 * i], fbuf.at[2 * i + 1], fs.at[2 * i + 1], fr.at[2 * i + 1], sibling
        )
    for i in range(7):
        start(ccopy[OTHERS[i]])
        start(fcopy[2 * i + 2])
    start(fcopy[1])
    for k in OTHERS[7:]:
        start(ccopy[k])

    def take(n):
        for k in PAIRS[n]:
            if k > 0 and k not in taken:
                taken.append(k)
                fcopy[k].wait_recv()
                if k % 2 == 0:
                    start(fcopy[k + 1])

    taken = []

    low = lax.broadcasted_iota(jnp.int32, (24, 128), 1) < 64

    def turn(value):
        return pltpu.roll(value, 64, 1)

    def unpack_centers(m):
        a, b = cbuf[2 * m], cbuf[2 * m + 1]
        lanes = pl.ds(m * 128, 128)
        coef = jnp.concatenate(
            [jnp.where(low, a[0:24], turn(b[0:24])), jnp.where(low, turn(a[0:24]), b[0:24])], axis=0
        )
        high, rest = split(coef * SCALE)
        chl[0:COLS, lanes] = high
        chl[COLS:96, lanes] = rest
        places = jnp.where(low[0:3], a[24:27], turn(b[24:27]))
        for axis in range(3):
            line = jnp.broadcast_to(places[axis : axis + 1], (128, 128))
            cb[axis, m * 128 : (m + 1) * 128, :] = line.T

    def unpack_fluid(n):
        for part in range(2):
            high, rest = split(fbuf[PAIRS[n][part], 0:COLS, :] * SCALE)
            lanes = pl.ds(part * 128, 128)
            fhl[n, 0:COLS, lanes] = high
            fhl[n, COLS:96, lanes] = rest

    def kernel_tile(half, n, kh, kl):
        places = [[fbuf[k, COLS + axis : COLS + axis + 1, :] for axis in range(3)] for k in PAIRS[n]]
        for first in range(0, HALF, STRIP):
            rows = pl.ds(half * HALF + first, STRIP)
            at = [cb[axis, rows, :] for axis in range(3)]
            for part in range(2):
                dx, dy, dz = (at[axis] - places[part][axis] for axis in range(3))
                sq = dx * dx + dy * dy + dz * dz
                inverse = lax.rsqrt(sq)
                turns = sq * inverse - 0.25
                b = 0.25 - jnp.abs(turns - jnp.round(turns))
                b2 = b * b
                value = b2 + S[3]
                for coefficient in (S[2], S[1], S[0]):
                    value = value * b2 + coefficient
                high, rest = split(value * (b * inverse))
                kh[first : first + STRIP, part * 128 : (part + 1) * 128] = high
                kl[first : first + STRIP, part * 128 : (part + 1) * 128] = rest

    def load_product(half, n, kh, kl):
        forces = fhl[n]
        across = (((1,), (1,)), ((), ()))
        load = lax.dot_general(kh[...], forces, across, preferred_element_type=F32)
        load += lax.dot_general(kl[...], forces, across, preferred_element_type=F32)
        if n == (FIRST if half == 0 else SECOND)[0]:
            lacc[half] = load
        else:
            lacc[half] += load

    def motion_product(half, n, kh, kl):
        coef = chl[:, half * HALF : (half + 1) * HALF]
        motion = jnp.dot(coef, kh[...], preferred_element_type=F32)
        motion += jnp.dot(coef, kl[...], preferred_element_type=F32)
        motion = motion[0:COLS] + motion[COLS:96]
        for part, k in enumerate(PAIRS[n]):
            piece = motion[:, part * 128 : (part + 1) * 128]
            if half == 0:
                macc[k] = piece
            else:
                macc[k] += piece

    def send_loads(half):
        total = lacc[half]
        total = (total + pltpu.roll(total, 80, 1)).T[0:COLS]
        for pair in range(4):
            m = half * 4 + pair
            piece = total[:, pair * 128 : (pair + 1) * 128]
            top, bottom = piece[0:24], piece[24:48]
            lsend[2 * m] = jnp.where(low, top, turn(bottom))
            lsend[2 * m + 1] = jnp.where(low, turn(top), bottom)
        for k in OTHERS:
            if k // 8 == half:
                dx, dy = PLANE[k]
                lcopy[k] = start(
                    remote(lsend.at[k], lrecv.at[k], ls.at[k], lr.at[k], plane_dev(4 - dx, 4 - dy))
                )

    lcopy, scopy, mcopy = {}, {}, {}

    def to_sibling(n):
        for k in PAIRS[n]:
            if k % 2:
                i = k // 2
                scopy[i] = start(remote(macc.at[k], msib.at[i], ss.at[i], sr.at[i], sibling))

    def to_owner(n):
        for k in PAIRS[n]:
            if k % 2 == 0 and k > 0:
                i = k // 2
                scopy[i].wait_recv()
                mout[i] = macc[k] + msib[i]
                mcopy[i] = start(
                    remote(mout.at[i], mrecv.at[i], ms.at[i], mr.at[i], line_dev(8 - LINE[i]))
                )

    buffers = ((kh0, kl0), (kh1, kl1))
    order = [(0, n) for n in FIRST] + [(1, n) for n in SECOND]
    take(0)
    take(1)
    for k in range(8):
        ccopy[k].wait_recv()
    for m in range(4):
        unpack_centers(m)
    for step, (half, n) in enumerate(order):
        if half == 0:
            take(n)
            unpack_fluid(n)
        if step == 5:
            for k in OTHERS[8:]:
                ccopy[k].wait_recv()
            for m in range(4, 8):
                unpack_centers(m)
        kernel_tile(half, n, *buffers[step % 2])
        if step > 0:
            load_product(*order[step - 1], *buffers[(step - 1) % 2])
            motion_product(*order[step - 1], *buffers[(step - 1) % 2])
        if step == TILES:
            send_loads(0)
        if step > TILES:
            to_sibling(order[step - 1][1])
            to_owner(order[step - 1][1])
    load_product(*order[-1], *buffers[(len(order) - 1) % 2])
    send_loads(1)
    motion_product(*order[-1], *buffers[(len(order) - 1) % 2])
    to_owner(0)

    motion = own[...] + macc[0]
    for i in range(1, 8):
        mcopy[i].wait_recv()
        motion += mrecv[i]
    scopy[0].wait_recv()
    motion_ref[...] = motion + msib[0]
    for k in OTHERS:
        lcopy[k].wait_recv()
    load = lsend[OWN]
    for k in OTHERS:
        load += lrecv[k]
    load_ref[0:24, :] = load[:, 0:64]
    load_ref[24:48, :] = load[:, 64:128]
    for copy in started:
        copy.wait_send()


def per_device(fluid_data, center_data, poly_coef):
    vmem = pl.BlockSpec(memory_space=pltpu.VMEM)
    hbm = pl.BlockSpec(memory_space=pltpu.HBM)
    dma = pltpu.SemaphoreType.DMA((16,))
    return pl.pallas_call(
        body,
        out_shape=(
            jax.ShapeDtypeStruct((COLS, 128), F32),
            jax.ShapeDtypeStruct((COLS, 64), F32),
        ),
        in_specs=[hbm] * 3,
        out_specs=(vmem, vmem),
        scratch_shapes=[
            pltpu.VMEM((51, 128), F32),
            pltpu.VMEM((51, 64), F32),
            pltpu.VMEM((4, COLS), F32),
            pltpu.VMEM((16, 51, 128), F32),
            pltpu.VMEM((16, 27, 128), F32),
            pltpu.VMEM((3, 1024, 128), F32),
            pltpu.VMEM((TILES, 128, 256), BF16),
            pltpu.VMEM((96, 1024), BF16),
            pltpu.VMEM((HALF, 256), BF16),
            pltpu.VMEM((HALF, 256), BF16),
            pltpu.VMEM((HALF, 256), BF16),
            pltpu.VMEM((HALF, 256), BF16),
            pltpu.VMEM((2, HALF, 128), F32),
            pltpu.VMEM((16, COLS, 128), F32),
            pltpu.VMEM((8, COLS, 128), F32),
            pltpu.VMEM((8, COLS, 128), F32),
            pltpu.VMEM((8, COLS, 128), F32),
            pltpu.VMEM((16, 24, 128), F32),
            pltpu.VMEM((16, 24, 128), F32),
            pltpu.VMEM((COLS, 128), F32),
            pltpu.SemaphoreType.DMA((3,)),
            *([dma] * 10),
        ],
        compiler_params=pltpu.CompilerParams(
            collective_id=0, has_side_effects=True, vmem_limit_bytes=24 * 2**20
        ),
        name="couple",
    )(
        *(
            pltpu.with_memory_space_constraint(array, pltpu.HBM)
            for array in (fluid_data, center_data, poly_coef.T)
        )
    )


def solution(mesh):
    return jax.shard_map(
        per_device,
        mesh=mesh,
        in_specs=(P(None, ("row", "col")), P(None, ("col", "row")), P()),
        out_specs=(P(None, ("row", "col")), P(None, ("col", "row"))),
        check_vma=False,
    )
```

```python
import jax
import jax.numpy as jnp
from jax import lax
from jax.experimental import pallas as pl
from jax.experimental.pallas import tpu as pltpu
from jax.sharding import PartitionSpec as P

WAVES = 64
COLS = 48
PLANE = [
    (2, 2), (1, 2), (3, 2), (2, 1), (2, 3), (3, 3), (3, 1), (1, 3),
    (0, 0), (1, 0), (3, 0), (0, 1), (0, 3), (2, 0), (0, 2), (1, 1),
]
OWN = 8
OTHERS = [0, 1, 2, 3, 4, 5, 6, 7, 15, 14, 13, 12, 11, 10, 9]
LINE = [0, 1, 7, 2, 6, 3, 5, 4]
PAIRS = [(0, 2), (4, 6), (8, 10), (12, 14), (1, 3), (5, 7), (9, 11), (13, 15)]
FIRST = [0, 1, 2, 3, 4, 5, 6, 7]
SECOND = [7, 6, 5, 4, 3, 2, 1, 0]
HALF = 512
TILES = 8
STRIP = 32
SCALE = 6.292462070004323
S = [s / SCALE for s in (0.9999999765898422, -6.57972875383963, 12.987203158835507, -12.183276227896942)]
F32 = jnp.float32
BF16 = jnp.bfloat16


def split(value):
    high = value.astype(BF16)
    return high, (value - high.astype(F32)).astype(BF16)


def body(
    fluid_hbm, center_hbm, poly_hbm, motion_ref, load_ref,
    fluid_ref, center_ref, poly_ref, fbuf, cbuf, cb, fhl, chl, kh0, kl0, kh1, kl1, lacc, macc, msib, mout, mrecv, lsend, lrecv, own,
    ins, fs, fr, cs, cr, ss, sr, ms, mr, ls, lr,
):
    row, col = lax.axis_index("row"), lax.axis_index("col")
    core, z_hi, y = row % 2, (row // 2) % 2, row // 4
    x, z_lo = col % 4, col // 4
    z = z_hi * 4 + z_lo

    def plane_dev(dx, dy):
        return {"row": (row + 4 * dy) % 16, "col": z_lo * 4 + (x + dx) % 4}

    def line_dev(dz, flip=0):
        z2 = (z + dz) % 8
        return {"row": 4 * y + 2 * (z2 // 4) + (core + flip) % 2, "col": (z2 % 4) * 4 + x}

    def remote(src, dst, send, recv, dev):
        return pltpu.make_async_remote_copy(
            src_ref=src, dst_ref=dst, send_sem=send, recv_sem=recv,
            device_id=dev, device_id_type=pl.DeviceIdType.MESH,
        )

    fetched = [
        pltpu.make_async_copy(source, target, ins.at[i])
        for i, (source, target) in enumerate(
            ((fluid_hbm, fluid_ref), (center_hbm, center_ref), (poly_hbm, poly_ref))
        )
    ]
    for copy in fetched:
        copy.start()
    sibling = line_dev(0, 1)
    barrier = pltpu.get_barrier_semaphore()
    peers = [plane_dev(*PLANE[k]) for k in OTHERS]
    peers += [line_dev(LINE[i]) for i in range(1, 8)] + [sibling]
    for dev in peers:
        pl.semaphore_signal(barrier, inc=1, device_id=dev, device_id_type=pl.DeviceIdType.MESH)

    for copy in fetched:
        copy.wait()

    fbuf[0, 0:COLS, :] = fluid_ref[3:51, :]
    fbuf[0, COLS:51, :] = fluid_ref[0:3, :] * WAVES
    cbuf[OWN, 0:24, 0:64] = center_ref[3:27, :]
    cbuf[OWN, 0:24, 64:128] = center_ref[27:51, :]
    cbuf[OWN, 24:27, :] = jnp.zeros((3, 128), F32)
    cbuf[OWN, 24:27, 0:64] = center_ref[0:3, :] * WAVES
    fhl[:, 96:128, :] = jnp.zeros((TILES, 32, 256), BF16)

    def poly_column(which):
        return jnp.broadcast_to(poly_ref[which : which + 1, :], (128, COLS)).T

    affine = poly_column(0)
    for axis in range(3):
        affine += poly_column(axis + 1) * fluid_ref[axis : axis + 1, :]
    own[...] = affine

    pl.semaphore_wait(barrier, len(peers))
    started = []

    def start(copy):
        copy.start()
        started.append(copy)
        return copy

    ccopy = {
        k: remote(cbuf.at[OWN], cbuf.at[k], cs.at[k], cr.at[k], plane_dev(*PLANE[k])) for k in OTHERS
    }
    fcopy = [None] * 16
    fcopy[1] = remote(fbuf.at[0], fbuf.at[1], fs.at[1], fr.at[1], sibling)
    for i in range(1, 8):
        fcopy[2 * i] = remote(
            fbuf.at[0], fbuf.at[2 * i], fs.at[2 * i], fr.at[2 * i], line_dev(LINE[i])
        )
        fcopy[2 * i + 1] = remote(
            fbuf.at[2 * i], fbuf.at[2 * i + 1], fs.at[2 * i + 1], fr.at[2 * i + 1], sibling
        )
    for i in range(7):
        start(ccopy[OTHERS[i]])
        start(fcopy[2 * i + 2])
    start(fcopy[1])
    for k in OTHERS[7:]:
        start(ccopy[k])

    def take(n):
        for k in PAIRS[n]:
            if k > 0 and k not in taken:
                taken.append(k)
                fcopy[k].wait_recv()
                if k % 2 == 0:
                    start(fcopy[k + 1])

    taken = []

    low = lax.broadcasted_iota(jnp.int32, (24, 128), 1) < 64

    def turn(value):
        return pltpu.roll(value, 64, 1)

    def unpack_centers(m):
        a, b = cbuf[2 * m], cbuf[2 * m + 1]
        lanes = pl.ds(m * 128, 128)
        coef = jnp.concatenate(
            [jnp.where(low, a[0:24], turn(b[0:24])), jnp.where(low, turn(a[0:24]), b[0:24])], axis=0
        )
        high, rest = split(coef * SCALE)
        chl[0:COLS, lanes] = high
        chl[COLS:96, lanes] = rest
        places = jnp.where(low[0:3], a[24:27], turn(b[24:27]))
        for axis in range(3):
            line = jnp.broadcast_to(places[axis : axis + 1], (128, 128))
            cb[axis, m * 128 : (m + 1) * 128, :] = line.T

    def unpack_fluid(n):
        for part in range(2):
            high, rest = split(fbuf[PAIRS[n][part], 0:COLS, :] * SCALE)
            lanes = pl.ds(part * 128, 128)
            fhl[n, 0:COLS, lanes] = high
            fhl[n, COLS:96, lanes] = rest

    def kernel_tile(half, n, kh, kl):
        places = [[fbuf[k, COLS + axis : COLS + axis + 1, :] for axis in range(3)] for k in PAIRS[n]]
        for first in range(0, HALF, STRIP):
            rows = pl.ds(half * HALF + first, STRIP)
            at = [cb[axis, rows, :] for axis in range(3)]
            for part in range(2):
                dx, dy, dz = (at[axis] - places[part][axis] for axis in range(3))
                sq = dx * dx + dy * dy + dz * dz
                inverse = lax.rsqrt(sq)
                turns = sq * inverse - 0.25
                b = 0.25 - jnp.abs(turns - jnp.round(turns))
                b2 = b * b
                value = b2 + S[3]
                for coefficient in (S[2], S[1], S[0]):
                    value = value * b2 + coefficient
                high, rest = split(value * (b * inverse))
                kh[first : first + STRIP, part * 128 : (part + 1) * 128] = high
                kl[first : first + STRIP, part * 128 : (part + 1) * 128] = rest

    def load_product(half, n, kh, kl):
        forces = fhl[n]
        across = (((1,), (1,)), ((), ()))
        load = lax.dot_general(kh[...], forces, across, preferred_element_type=F32)
        load += lax.dot_general(kl[...], forces, across, preferred_element_type=F32)
        if n == (FIRST if half == 0 else SECOND)[0]:
            lacc[half] = load
        else:
            lacc[half] += load

    def motion_product(half, n, kh, kl):
        coef = chl[:, half * HALF : (half + 1) * HALF]
        motion = jnp.dot(coef, kh[...], preferred_element_type=F32)
        motion += jnp.dot(coef, kl[...], preferred_element_type=F32)
        motion = motion[0:COLS] + motion[COLS:96]
        for part, k in enumerate(PAIRS[n]):
            piece = motion[:, part * 128 : (part + 1) * 128]
            if half == 0:
                macc[k] = piece
            else:
                macc[k] += piece

    def send_loads(half):
        total = lacc[half]
        total = (total + pltpu.roll(total, 80, 1)).T[0:COLS]
        for pair in range(4):
            m = half * 4 + pair
            piece = total[:, pair * 128 : (pair + 1) * 128]
            top, bottom = piece[0:24], piece[24:48]
            lsend[2 * m] = jnp.where(low, top, turn(bottom))
            lsend[2 * m + 1] = jnp.where(low, turn(top), bottom)
        for k in OTHERS:
            if k // 8 == half:
                dx, dy = PLANE[k]
                lcopy[k] = start(
                    remote(lsend.at[k], lrecv.at[k], ls.at[k], lr.at[k], plane_dev(4 - dx, 4 - dy))
                )

    lcopy, scopy, mcopy = {}, {}, {}

    def to_sibling(n):
        for k in PAIRS[n]:
            if k % 2:
                i = k // 2
                scopy[i] = start(remote(macc.at[k], msib.at[i], ss.at[i], sr.at[i], sibling))

    def to_owner(n):
        for k in PAIRS[n]:
            if k % 2 == 0 and k > 0:
                i = k // 2
                scopy[i].wait_recv()
                mout[i] = macc[k] + msib[i]
                mcopy[i] = start(
                    remote(mout.at[i], mrecv.at[i], ms.at[i], mr.at[i], line_dev(8 - LINE[i]))
                )

    buffers = ((kh0, kl0), (kh1, kl1))
    order = [(0, n) for n in FIRST] + [(1, n) for n in SECOND]
    take(0)
    take(1)
    for k in range(8):
        ccopy[k].wait_recv()
    for m in range(4):
        unpack_centers(m)
    for step in range(0, 16, 2):
        if step < TILES:
            for half, n in order[step : step + 2]:
                take(n)
                unpack_fluid(n)
        if step == 4:
            for k in OTHERS[8:]:
                ccopy[k].wait_recv()
            for m in range(4, 8):
                unpack_centers(m)
        for each in (step, step + 1):
            kernel_tile(*order[each], *buffers[each % 2])
            if each > 0:
                load_product(*order[each - 1], *buffers[(each - 1) % 2])
                motion_product(*order[each - 1], *buffers[(each - 1) % 2])
        if step == TILES:
            send_loads(0)
        for each in (step - 1, step):
            if each >= TILES:
                to_sibling(order[each][1])
                to_owner(order[each][1])
    load_product(*order[-1], *buffers[(len(order) - 1) % 2])
    send_loads(1)
    motion_product(*order[-1], *buffers[(len(order) - 1) % 2])
    early = len(started) - 7
    to_owner(0)
    for copy in started[:early]:
        copy.wait_send()

    motion = own[...] + macc[0]
    for i in range(1, 8):
        mcopy[i].wait_recv()
        motion += mrecv[i]
    scopy[0].wait_recv()
    motion_ref[...] = motion + msib[0]
    for k in OTHERS:
        lcopy[k].wait_recv()
    load = lsend[OWN]
    for k in OTHERS:
        load += lrecv[k]
    load_ref[0:24, :] = load[:, 0:64]
    load_ref[24:48, :] = load[:, 64:128]
    for copy in started[early:]:
        copy.wait_send()


def deliver(motion_ref, load_ref, motion_out, load_out, sems):
    copies = [
        pltpu.make_async_copy(motion_ref, motion_out, sems.at[0]),
        pltpu.make_async_copy(load_ref, load_out, sems.at[1]),
    ]
    for copy in copies:
        copy.start()
    for copy in copies:
        copy.wait()


def per_device(fluid_data, center_data, poly_coef):
    vmem = pl.BlockSpec(memory_space=pltpu.VMEM)
    hbm = pl.BlockSpec(memory_space=pltpu.HBM)
    dma = pltpu.SemaphoreType.DMA((16,))
    shapes = (
        jax.ShapeDtypeStruct((COLS, 128), F32),
        jax.ShapeDtypeStruct((COLS, 64), F32),
    )
    outputs = pl.pallas_call(
        body,
        out_shape=shapes,
        in_specs=[hbm] * 3,
        out_specs=(vmem, vmem),
        scratch_shapes=[
            pltpu.VMEM((51, 128), F32),
            pltpu.VMEM((51, 64), F32),
            pltpu.VMEM((4, COLS), F32),
            pltpu.VMEM((16, 51, 128), F32),
            pltpu.VMEM((16, 27, 128), F32),
            pltpu.VMEM((3, 1024, 128), F32),
            pltpu.VMEM((TILES, 128, 256), BF16),
            pltpu.VMEM((96, 1024), BF16),
            pltpu.VMEM((HALF, 256), BF16),
            pltpu.VMEM((HALF, 256), BF16),
            pltpu.VMEM((HALF, 256), BF16),
            pltpu.VMEM((HALF, 256), BF16),
            pltpu.VMEM((2, HALF, 128), F32),
            pltpu.VMEM((16, COLS, 128), F32),
            pltpu.VMEM((8, COLS, 128), F32),
            pltpu.VMEM((8, COLS, 128), F32),
            pltpu.VMEM((8, COLS, 128), F32),
            pltpu.VMEM((16, 24, 128), F32),
            pltpu.VMEM((16, 24, 128), F32),
            pltpu.VMEM((COLS, 128), F32),
            pltpu.SemaphoreType.DMA((3,)),
            *([dma] * 10),
        ],
        compiler_params=pltpu.CompilerParams(
            collective_id=0, has_side_effects=True, vmem_limit_bytes=24 * 2**20
        ),
        name="couple",
    )(
        *(
            pltpu.with_memory_space_constraint(array, pltpu.HBM)
            for array in (fluid_data, center_data, poly_coef.T)
        )
    )
    return pl.pallas_call(
        deliver,
        out_shape=shapes,
        in_specs=[vmem] * 2,
        out_specs=(hbm, hbm),
        scratch_shapes=[pltpu.SemaphoreType.DMA((2,))],
        compiler_params=pltpu.CompilerParams(vmem_limit_bytes=2**20),
        name="deliver",
    )(*outputs)


def solution(mesh):
    return jax.shard_map(
        per_device,
        mesh=mesh,
        in_specs=(P(None, ("row", "col")), P(None, ("col", "row")), P()),
        out_specs=(P(None, ("row", "col")), P(None, ("col", "row"))),
        check_vma=False,
    )
```

```python
import jax
import jax.numpy as jnp
from jax import lax
from jax.experimental import pallas as pl
from jax.experimental.pallas import tpu as pltpu
from jax.sharding import PartitionSpec as P

WAVES = 64
COLS = 48
PLANE = [
    (2, 2), (1, 2), (3, 2), (2, 1), (2, 3), (3, 3), (3, 1), (1, 3),
    (0, 0), (1, 0), (3, 0), (0, 1), (0, 3), (2, 0), (0, 2), (1, 1),
]
OWN = 8
OTHERS = [0, 1, 2, 3, 4, 5, 6, 7, 15, 14, 13, 12, 11, 10, 9]
LINE = [0, 1, 7, 2, 6, 3, 5, 4]
PAIRS = [(0, 2), (4, 6), (8, 10), (12, 14), (1, 3), (5, 7), (9, 11), (13, 15)]
FIRST = [0, 1, 2, 3, 4, 5, 6, 7]
SECOND = [7, 6, 5, 4, 3, 2, 1, 0]
HALF = 512
TILES = 8
STRIP = 32
SCALE = 6.292462070004323
S = [s / SCALE for s in (0.9999999765898422, -6.57972875383963, 12.987203158835507, -12.183276227896942)]
F32 = jnp.float32
BF16 = jnp.bfloat16


def split(value):
    high = value.astype(BF16)
    return high, (value - high.astype(F32)).astype(BF16)


def body(
    fluid_hbm, center_hbm, poly_hbm, motion_ref, load_ref,
    fluid_ref, center_ref, poly_ref, fbuf, cbuf, cb, fhl, chl, kh0, kl0, kh1, kl1, lacc, macc, msib, mout, mrecv, lsend, lrecv, own,
    ins, fs, fr, cs, cr, ss, sr, ms, mr, ls, lr,
):
    row, col = lax.axis_index("row"), lax.axis_index("col")
    core, z_hi, y = row % 2, (row // 2) % 2, row // 4
    x, z_lo = col % 4, col // 4
    z = z_hi * 4 + z_lo

    def plane_dev(dx, dy):
        return {"row": (row + 4 * dy) % 16, "col": z_lo * 4 + (x + dx) % 4}

    def line_dev(dz, flip=0):
        z2 = (z + dz) % 8
        return {"row": 4 * y + 2 * (z2 // 4) + (core + flip) % 2, "col": (z2 % 4) * 4 + x}

    def remote(src, dst, send, recv, dev):
        return pltpu.make_async_remote_copy(
            src_ref=src, dst_ref=dst, send_sem=send, recv_sem=recv,
            device_id=dev, device_id_type=pl.DeviceIdType.MESH,
        )

    fetched = [
        pltpu.make_async_copy(source, target, ins.at[i])
        for i, (source, target) in enumerate(
            ((fluid_hbm, fluid_ref), (center_hbm, center_ref), (poly_hbm, poly_ref))
        )
    ]
    for copy in fetched:
        copy.start()
    sibling = line_dev(0, 1)
    barrier = pltpu.get_barrier_semaphore()
    peers = [plane_dev(*PLANE[k]) for k in OTHERS]
    peers += [line_dev(LINE[i]) for i in range(1, 8)] + [sibling]
    for dev in peers:
        pl.semaphore_signal(barrier, inc=1, device_id=dev, device_id_type=pl.DeviceIdType.MESH)

    for copy in fetched:
        copy.wait()

    fbuf[0, 0:COLS, :] = fluid_ref[3:51, :]
    fbuf[0, COLS:51, :] = fluid_ref[0:3, :] * WAVES
    cbuf[OWN, 0:24, 0:64] = center_ref[3:27, :]
    cbuf[OWN, 0:24, 64:128] = center_ref[27:51, :]
    cbuf[OWN, 24:27, :] = jnp.zeros((3, 128), F32)
    cbuf[OWN, 24:27, 0:64] = center_ref[0:3, :] * WAVES
    fhl[:, 96:128, :] = jnp.zeros((TILES, 32, 256), BF16)

    def poly_column(which):
        return jnp.broadcast_to(poly_ref[which : which + 1, :], (128, COLS)).T

    affine = poly_column(0)
    for axis in range(3):
        affine += poly_column(axis + 1) * fluid_ref[axis : axis + 1, :]
    own[...] = affine

    pl.semaphore_wait(barrier, len(peers))
    started = []

    def start(copy):
        copy.start()
        started.append(copy)
        return copy

    ccopy = {
        k: remote(cbuf.at[OWN], cbuf.at[k], cs.at[k], cr.at[k], plane_dev(*PLANE[k])) for k in OTHERS
    }
    fcopy = [None] * 16
    fcopy[1] = remote(fbuf.at[0], fbuf.at[1], fs.at[1], fr.at[1], sibling)
    for i in range(1, 8):
        fcopy[2 * i] = remote(
            fbuf.at[0], fbuf.at[2 * i], fs.at[2 * i], fr.at[2 * i], line_dev(LINE[i])
        )
        fcopy[2 * i + 1] = remote(
            fbuf.at[2 * i], fbuf.at[2 * i + 1], fs.at[2 * i + 1], fr.at[2 * i + 1], sibling
        )
    start(fcopy[1])
    for i in range(7):
        start(ccopy[OTHERS[i]])
        start(fcopy[2 * i + 2])
    for k in OTHERS[7:]:
        start(ccopy[k])

    def take(n):
        for k in PAIRS[n]:
            if k > 0 and k not in taken:
                taken.append(k)
                fcopy[k].wait_recv()
                if k % 2 == 0:
                    start(fcopy[k + 1])

    taken = []

    low = lax.broadcasted_iota(jnp.int32, (24, 128), 1) < 64

    def turn(value):
        return pltpu.roll(value, 64, 1)

    def unpack_centers(m):
        a, b = cbuf[2 * m], cbuf[2 * m + 1]
        lanes = pl.ds(m * 128, 128)
        coef = jnp.concatenate(
            [jnp.where(low, a[0:24], turn(b[0:24])), jnp.where(low, turn(a[0:24]), b[0:24])], axis=0
        )
        high, rest = split(coef * SCALE)
        chl[0:COLS, lanes] = high
        chl[COLS:96, lanes] = rest
        places = jnp.where(low[0:3], a[24:27], turn(b[24:27]))
        for axis in range(3):
            line = jnp.broadcast_to(places[axis : axis + 1], (128, 128))
            cb[axis, m * 128 : (m + 1) * 128, :] = line.T

    def unpack_fluid(n):
        for part in range(2):
            high, rest = split(fbuf[PAIRS[n][part], 0:COLS, :] * SCALE)
            lanes = pl.ds(part * 128, 128)
            fhl[n, 0:COLS, lanes] = high
            fhl[n, COLS:96, lanes] = rest

    def kernel_tile(half, n, kh, kl):
        places = [[fbuf[k, COLS + axis : COLS + axis + 1, :] for axis in range(3)] for k in PAIRS[n]]
        for first in range(0, HALF, STRIP):
            rows = pl.ds(half * HALF + first, STRIP)
            at = [cb[axis, rows, :] for axis in range(3)]
            for part in range(2):
                dx, dy, dz = (at[axis] - places[part][axis] for axis in range(3))
                sq = dx * dx + dy * dy + dz * dz
                inverse = lax.rsqrt(sq)
                turns = sq * inverse - 0.25
                b = 0.25 - jnp.abs(turns - jnp.round(turns))
                b2 = b * b
                value = b2 + S[3]
                for coefficient in (S[2], S[1], S[0]):
                    value = value * b2 + coefficient
                high, rest = split(value * (b * inverse))
                kh[first : first + STRIP, part * 128 : (part + 1) * 128] = high
                kl[first : first + STRIP, part * 128 : (part + 1) * 128] = rest

    def load_product(half, n, kh, kl):
        forces = fhl[n]
        across = (((1,), (1,)), ((), ()))
        load = lax.dot_general(kh[...], forces, across, preferred_element_type=F32)
        load += lax.dot_general(kl[...], forces, across, preferred_element_type=F32)
        if n == (FIRST if half == 0 else SECOND)[0]:
            lacc[half] = load
        else:
            lacc[half] += load

    def motion_product(half, n, kh, kl):
        coef = chl[:, half * HALF : (half + 1) * HALF]
        motion = jnp.dot(coef, kh[...], preferred_element_type=F32)
        motion += jnp.dot(coef, kl[...], preferred_element_type=F32)
        motion = motion[0:COLS] + motion[COLS:96]
        for part, k in enumerate(PAIRS[n]):
            piece = motion[:, part * 128 : (part + 1) * 128]
            if half == 0:
                macc[k] = piece
            else:
                macc[k] += piece

    def send_loads(half):
        total = lacc[half]
        total = (total + pltpu.roll(total, 80, 1)).T[0:COLS]
        for pair in range(4):
            m = half * 4 + pair
            piece = total[:, pair * 128 : (pair + 1) * 128]
            top, bottom = piece[0:24], piece[24:48]
            lsend[2 * m] = jnp.where(low, top, turn(bottom))
            lsend[2 * m + 1] = jnp.where(low, turn(top), bottom)
        for k in OTHERS:
            if k // 8 == half:
                dx, dy = PLANE[k]
                lcopy[k] = start(
                    remote(lsend.at[k], lrecv.at[k], ls.at[k], lr.at[k], plane_dev(4 - dx, 4 - dy))
                )

    lcopy, scopy, mcopy = {}, {}, {}

    def to_sibling(n):
        for k in PAIRS[n]:
            if k % 2:
                i = k // 2
                scopy[i] = start(remote(macc.at[k], msib.at[i], ss.at[i], sr.at[i], sibling))

    def to_owner(n):
        for k in PAIRS[n]:
            if k % 2 == 0 and k > 0:
                i = k // 2
                scopy[i].wait_recv()
                mout[i] = macc[k] + msib[i]
                mcopy[i] = start(
                    remote(mout.at[i], mrecv.at[i], ms.at[i], mr.at[i], line_dev(8 - LINE[i]))
                )

    buffers = ((kh0, kl0), (kh1, kl1))
    order = [(0, n) for n in FIRST] + [(1, n) for n in SECOND]
    take(0)
    for k in range(8):
        ccopy[k].wait_recv()
    for m in range(4):
        unpack_centers(m)
    for step in range(0, 16, 2):
        if step < TILES:
            for half, n in order[step : step + 2]:
                take(n)
                unpack_fluid(n)
        if step == 4:
            for k in OTHERS[8:]:
                ccopy[k].wait_recv()
            for m in range(4, 8):
                unpack_centers(m)
        for each in (step, step + 1):
            kernel_tile(*order[each], *buffers[each % 2])
            if each > 0:
                load_product(*order[each - 1], *buffers[(each - 1) % 2])
                motion_product(*order[each - 1], *buffers[(each - 1) % 2])
        if step == TILES + 4:
            send_loads(0)
        for each in (step - 1, step):
            if each >= TILES:
                to_sibling(order[each][1])
                to_owner(order[each][1])
    load_product(*order[-1], *buffers[(len(order) - 1) % 2])
    send_loads(1)
    motion_product(*order[-1], *buffers[(len(order) - 1) % 2])
    early = len(started) - 7
    to_owner(0)
    for copy in started[:early]:
        copy.wait_send()

    motion = own[...] + macc[0]
    for i in range(1, 8):
        mcopy[i].wait_recv()
        motion += mrecv[i]
    scopy[0].wait_recv()
    motion_ref[...] = motion + msib[0]
    for k in OTHERS:
        lcopy[k].wait_recv()
    load = lsend[OWN]
    for k in OTHERS:
        load += lrecv[k]
    load_ref[0:24, :] = load[:, 0:64]
    load_ref[24:48, :] = load[:, 64:128]
    for copy in started[early:]:
        copy.wait_send()


def deliver(motion_ref, load_ref, motion_out, load_out, sems):
    copies = [
        pltpu.make_async_copy(motion_ref, motion_out, sems.at[0]),
        pltpu.make_async_copy(load_ref, load_out, sems.at[1]),
    ]
    for copy in copies:
        copy.start()
    for copy in copies:
        copy.wait()


def per_device(fluid_data, center_data, poly_coef):
    vmem = pl.BlockSpec(memory_space=pltpu.VMEM)
    hbm = pl.BlockSpec(memory_space=pltpu.HBM)
    dma = pltpu.SemaphoreType.DMA((16,))
    shapes = (
        jax.ShapeDtypeStruct((COLS, 128), F32),
        jax.ShapeDtypeStruct((COLS, 64), F32),
    )
    outputs = pl.pallas_call(
        body,
        out_shape=shapes,
        in_specs=[hbm] * 3,
        out_specs=(vmem, vmem),
        scratch_shapes=[
            pltpu.VMEM((51, 128), F32),
            pltpu.VMEM((51, 64), F32),
            pltpu.VMEM((4, COLS), F32),
            pltpu.VMEM((16, 51, 128), F32),
            pltpu.VMEM((16, 27, 128), F32),
            pltpu.VMEM((3, 1024, 128), F32),
            pltpu.VMEM((TILES, 128, 256), BF16),
            pltpu.VMEM((96, 1024), BF16),
            pltpu.VMEM((HALF, 256), BF16),
            pltpu.VMEM((HALF, 256), BF16),
            pltpu.VMEM((HALF, 256), BF16),
            pltpu.VMEM((HALF, 256), BF16),
            pltpu.VMEM((2, HALF, 128), F32),
            pltpu.VMEM((16, COLS, 128), F32),
            pltpu.VMEM((8, COLS, 128), F32),
            pltpu.VMEM((8, COLS, 128), F32),
            pltpu.VMEM((8, COLS, 128), F32),
            pltpu.VMEM((16, 24, 128), F32),
            pltpu.VMEM((16, 24, 128), F32),
            pltpu.VMEM((COLS, 128), F32),
            pltpu.SemaphoreType.DMA((3,)),
            *([dma] * 10),
        ],
        compiler_params=pltpu.CompilerParams(
            collective_id=0, has_side_effects=True, vmem_limit_bytes=24 * 2**20
        ),
        name="couple",
    )(
        *(
            pltpu.with_memory_space_constraint(array, pltpu.HBM)
            for array in (fluid_data, center_data, poly_coef.T)
        )
    )
    return pl.pallas_call(
        deliver,
        out_shape=shapes,
        in_specs=[vmem] * 2,
        out_specs=(hbm, hbm),
        scratch_shapes=[pltpu.SemaphoreType.DMA((2,))],
        compiler_params=pltpu.CompilerParams(vmem_limit_bytes=2**20),
        name="deliver",
    )(*outputs)


def solution(mesh):
    return jax.shard_map(
        per_device,
        mesh=mesh,
        in_specs=(P(None, ("row", "col")), P(None, ("col", "row")), P()),
        out_specs=(P(None, ("row", "col")), P(None, ("col", "row"))),
        check_vma=False,
    )
```

```python
import jax
import jax.numpy as jnp
from jax import lax
from jax.experimental import pallas as pl
from jax.experimental.pallas import tpu as pltpu
from jax.sharding import PartitionSpec as P

WAVES = 64
COLS = 48
PLANE = [
    (2, 2), (1, 2), (3, 2), (2, 1), (2, 3), (3, 3), (3, 1), (1, 3),
    (0, 0), (1, 0), (3, 0), (0, 1), (0, 3), (2, 0), (0, 2), (1, 1),
]
OWN = 8
OTHERS = [0, 1, 2, 3, 4, 5, 6, 7, 15, 14, 13, 12, 11, 10, 9]
LINE = [0, 1, 7, 2, 6, 3, 5, 4]
PAIRS = [(0, 2), (4, 6), (8, 10), (12, 14), (1, 3), (5, 7), (9, 11), (13, 15)]
FIRST = [0, 1, 2, 3, 4, 5, 6, 7]
SECOND = [7, 6, 5, 4, 3, 2, 1, 0]
HALF = 512
TILES = 8
STRIP = 32
SCALE = 6.292462070004323
S = [s / SCALE for s in (0.9999999765898422, -6.57972875383963, 12.987203158835507, -12.183276227896942)]
F32 = jnp.float32
BF16 = jnp.bfloat16


def split(value):
    high = value.astype(BF16)
    return high, (value - high.astype(F32)).astype(BF16)


def body(
    fluid_hbm, center_hbm, poly_hbm, motion_ref, load_ref,
    fluid_ref, center_ref, poly_ref, fbuf, cbuf, cb, fhl, chl, kh0, kl0, kh1, kl1, lacc, macc, msib, mout, mrecv, lsend, lrecv, own,
    ins, fs, fr, cs, cr, ss, sr, ms, mr, ls, lr,
):
    row, col = lax.axis_index("row"), lax.axis_index("col")
    core, z_hi, y = row % 2, (row // 2) % 2, row // 4
    x, z_lo = col % 4, col // 4
    z = z_hi * 4 + z_lo

    def plane_dev(dx, dy):
        return {"row": (row + 4 * dy) % 16, "col": z_lo * 4 + (x + dx) % 4}

    def line_dev(dz, flip=0):
        z2 = (z + dz) % 8
        return {"row": 4 * y + 2 * (z2 // 4) + (core + flip) % 2, "col": (z2 % 4) * 4 + x}

    def remote(src, dst, send, recv, dev):
        return pltpu.make_async_remote_copy(
            src_ref=src, dst_ref=dst, send_sem=send, recv_sem=recv,
            device_id=dev, device_id_type=pl.DeviceIdType.MESH,
        )

    fetched = [
        pltpu.make_async_copy(source, target, ins.at[i])
        for i, (source, target) in enumerate(
            ((fluid_hbm, fluid_ref), (center_hbm, center_ref), (poly_hbm, poly_ref))
        )
    ]
    for copy in fetched:
        copy.start()
    sibling = line_dev(0, 1)
    barrier = pltpu.get_barrier_semaphore()
    peers = [line_dev(LINE[i]) for i in reversed(range(1, 8))]
    peers += [plane_dev(*PLANE[k]) for k in OTHERS] + [sibling]
    for dev in peers:
        pl.semaphore_signal(barrier, inc=1, device_id=dev, device_id_type=pl.DeviceIdType.MESH)

    for copy in fetched:
        copy.wait()

    fbuf[0, 0:COLS, :] = fluid_ref[3:51, :]
    fbuf[0, COLS:51, :] = fluid_ref[0:3, :] * WAVES
    cbuf[OWN, 0:24, 0:64] = center_ref[3:27, :]
    cbuf[OWN, 0:24, 64:128] = center_ref[27:51, :]
    cbuf[OWN, 24:27, :] = jnp.zeros((3, 128), F32)
    cbuf[OWN, 24:27, 0:64] = center_ref[0:3, :] * WAVES
    fhl[:, 96:128, :] = jnp.zeros((TILES, 32, 256), BF16)

    def poly_column(which):
        return jnp.broadcast_to(poly_ref[which : which + 1, :], (128, COLS)).T

    affine = poly_column(0)
    for axis in range(3):
        affine += poly_column(axis + 1) * fluid_ref[axis : axis + 1, :]
    own[...] = affine

    pl.semaphore_wait(barrier, len(peers))
    started = []

    def start(copy):
        copy.start()
        started.append(copy)
        return copy

    ccopy = {
        k: remote(cbuf.at[OWN], cbuf.at[k], cs.at[k], cr.at[k], plane_dev(*PLANE[k])) for k in OTHERS
    }
    fcopy = [None] * 16
    fcopy[1] = remote(fbuf.at[0], fbuf.at[1], fs.at[1], fr.at[1], sibling)
    for i in range(1, 8):
        fcopy[2 * i] = remote(
            fbuf.at[0], fbuf.at[2 * i], fs.at[2 * i], fr.at[2 * i], line_dev(LINE[i])
        )
        fcopy[2 * i + 1] = remote(
            fbuf.at[2 * i], fbuf.at[2 * i + 1], fs.at[2 * i + 1], fr.at[2 * i + 1], sibling
        )
    start(fcopy[1])
    for i in range(7):
        start(ccopy[OTHERS[i]])
        start(fcopy[2 * i + 2])
    for k in OTHERS[7:]:
        start(ccopy[k])

    def take(n):
        for k in PAIRS[n]:
            if k > 0 and k not in taken:
                taken.append(k)
                fcopy[k].wait_recv()
                if k % 2 == 0:
                    start(fcopy[k + 1])

    taken = []

    low = lax.broadcasted_iota(jnp.int32, (24, 128), 1) < 64

    def turn(value):
        return pltpu.roll(value, 64, 1)

    def unpack_centers(m):
        a, b = cbuf[2 * m], cbuf[2 * m + 1]
        lanes = pl.ds(m * 128, 128)
        coef = jnp.concatenate(
            [jnp.where(low, a[0:24], turn(b[0:24])), jnp.where(low, turn(a[0:24]), b[0:24])], axis=0
        )
        high, rest = split(coef * SCALE)
        chl[0:COLS, lanes] = high
        chl[COLS:96, lanes] = rest
        places = jnp.where(low[0:3], a[24:27], turn(b[24:27]))
        for axis in range(3):
            line = jnp.broadcast_to(places[axis : axis + 1], (128, 128))
            cb[axis, m * 128 : (m + 1) * 128, :] = line.T

    def unpack_fluid(n):
        for part in range(2):
            high, rest = split(fbuf[PAIRS[n][part], 0:COLS, :] * SCALE)
            lanes = pl.ds(part * 128, 128)
            fhl[n, 0:COLS, lanes] = high
            fhl[n, COLS:96, lanes] = rest

    def kernel_tile(half, n, kh, kl):
        places = [[fbuf[k, COLS + axis : COLS + axis + 1, :] for axis in range(3)] for k in PAIRS[n]]
        for first in range(0, HALF, STRIP):
            rows = pl.ds(half * HALF + first, STRIP)
            at = [cb[axis, rows, :] for axis in range(3)]
            for part in range(2):
                dx, dy, dz = (at[axis] - places[part][axis] for axis in range(3))
                sq = dx * dx + dy * dy + dz * dz
                inverse = lax.rsqrt(sq)
                turns = sq * inverse - 0.25
                b = 0.25 - jnp.abs(turns - jnp.round(turns))
                b2 = b * b
                value = b2 + S[3]
                for coefficient in (S[2], S[1], S[0]):
                    value = value * b2 + coefficient
                high, rest = split(value * (b * inverse))
                kh[first : first + STRIP, part * 128 : (part + 1) * 128] = high
                kl[first : first + STRIP, part * 128 : (part + 1) * 128] = rest

    def load_product(half, n, kh, kl):
        forces = fhl[n]
        across = (((1,), (1,)), ((), ()))
        load = lax.dot_general(kh[...], forces, across, preferred_element_type=F32)
        load += lax.dot_general(kl[...], forces, across, preferred_element_type=F32)
        if n == (FIRST if half == 0 else SECOND)[0]:
            lacc[half] = load
        else:
            lacc[half] += load

    def motion_product(half, n, kh, kl):
        coef = chl[:, half * HALF : (half + 1) * HALF]
        motion = jnp.dot(coef, kh[...], preferred_element_type=F32)
        motion += jnp.dot(coef, kl[...], preferred_element_type=F32)
        motion = motion[0:COLS] + motion[COLS:96]
        for part, k in enumerate(PAIRS[n]):
            piece = motion[:, part * 128 : (part + 1) * 128]
            if half == 0:
                macc[k] = piece
            else:
                macc[k] += piece

    def send_loads(half):
        total = lacc[half]
        total = (total + pltpu.roll(total, 80, 1)).T[0:COLS]
        for pair in range(4):
            m = half * 4 + pair
            piece = total[:, pair * 128 : (pair + 1) * 128]
            top, bottom = piece[0:24], piece[24:48]
            lsend[2 * m] = jnp.where(low, top, turn(bottom))
            lsend[2 * m + 1] = jnp.where(low, turn(top), bottom)
        for k in OTHERS:
            if k // 8 == half:
                dx, dy = PLANE[k]
                lcopy[k] = start(
                    remote(lsend.at[k], lrecv.at[k], ls.at[k], lr.at[k], plane_dev(4 - dx, 4 - dy))
                )

    lcopy, scopy, mcopy = {}, {}, {}

    def to_sibling(n):
        for k in PAIRS[n]:
            if k % 2:
                i = k // 2
                scopy[i] = start(remote(macc.at[k], msib.at[i], ss.at[i], sr.at[i], sibling))

    def to_owner(n):
        for k in PAIRS[n]:
            if k % 2 == 0 and k > 0:
                i = k // 2
                scopy[i].wait_recv()
                mout[i] = macc[k] + msib[i]
                mcopy[i] = start(
                    remote(mout.at[i], mrecv.at[i], ms.at[i], mr.at[i], line_dev(8 - LINE[i]))
                )

    buffers = ((kh0, kl0), (kh1, kl1))
    order = [(0, n) for n in FIRST] + [(1, n) for n in SECOND]
    take(0)
    for k in range(8):
        ccopy[k].wait_recv()
    for m in range(4):
        unpack_centers(m)
    for step in range(0, 16, 2):
        if step < TILES:
            for half, n in order[step : step + 2]:
                take(n)
                unpack_fluid(n)
        if step == 4:
            for k in OTHERS[8:]:
                ccopy[k].wait_recv()
            for m in range(4, 8):
                unpack_centers(m)
        for each in (step, step + 1):
            kernel_tile(*order[each], *buffers[each % 2])
            if each > 0:
                load_product(*order[each - 1], *buffers[(each - 1) % 2])
                motion_product(*order[each - 1], *buffers[(each - 1) % 2])
        if step == TILES + 4:
            send_loads(0)
        for each in (step - 1, step):
            if each >= TILES:
                to_sibling(order[each][1])
                to_owner(order[each][1])
    load_product(*order[-1], *buffers[(len(order) - 1) % 2])
    send_loads(1)
    motion_product(*order[-1], *buffers[(len(order) - 1) % 2])
    early = len(started) - 7
    to_owner(0)
    for copy in started[:early]:
        copy.wait_send()

    motion = own[...] + macc[0]
    for i in range(1, 8):
        mcopy[i].wait_recv()
        motion += mrecv[i]
    scopy[0].wait_recv()
    motion_ref[...] = motion + msib[0]
    for k in OTHERS:
        lcopy[k].wait_recv()
    load = lsend[OWN]
    for k in OTHERS:
        load += lrecv[k]
    load_ref[0:24, :] = load[:, 0:64]
    load_ref[24:48, :] = load[:, 64:128]
    for copy in started[early:]:
        copy.wait_send()


def deliver(motion_ref, load_ref, motion_out, load_out, sems):
    copies = [
        pltpu.make_async_copy(motion_ref, motion_out, sems.at[0]),
        pltpu.make_async_copy(load_ref, load_out, sems.at[1]),
    ]
    for copy in copies:
        copy.start()
    for copy in copies:
        copy.wait()


def per_device(fluid_data, center_data, poly_coef):
    vmem = pl.BlockSpec(memory_space=pltpu.VMEM)
    hbm = pl.BlockSpec(memory_space=pltpu.HBM)
    dma = pltpu.SemaphoreType.DMA((16,))
    shapes = (
        jax.ShapeDtypeStruct((COLS, 128), F32),
        jax.ShapeDtypeStruct((COLS, 64), F32),
    )
    outputs = pl.pallas_call(
        body,
        out_shape=shapes,
        in_specs=[hbm] * 3,
        out_specs=(vmem, vmem),
        scratch_shapes=[
            pltpu.VMEM((51, 128), F32),
            pltpu.VMEM((51, 64), F32),
            pltpu.VMEM((4, COLS), F32),
            pltpu.VMEM((16, 51, 128), F32),
            pltpu.VMEM((16, 27, 128), F32),
            pltpu.VMEM((3, 1024, 128), F32),
            pltpu.VMEM((TILES, 128, 256), BF16),
            pltpu.VMEM((96, 1024), BF16),
            pltpu.VMEM((HALF, 256), BF16),
            pltpu.VMEM((HALF, 256), BF16),
            pltpu.VMEM((HALF, 256), BF16),
            pltpu.VMEM((HALF, 256), BF16),
            pltpu.VMEM((2, HALF, 128), F32),
            pltpu.VMEM((16, COLS, 128), F32),
            pltpu.VMEM((8, COLS, 128), F32),
            pltpu.VMEM((8, COLS, 128), F32),
            pltpu.VMEM((8, COLS, 128), F32),
            pltpu.VMEM((16, 24, 128), F32),
            pltpu.VMEM((16, 24, 128), F32),
            pltpu.VMEM((COLS, 128), F32),
            pltpu.SemaphoreType.DMA((3,)),
            *([dma] * 10),
        ],
        compiler_params=pltpu.CompilerParams(
            collective_id=0, has_side_effects=True, vmem_limit_bytes=24 * 2**20
        ),
        name="couple",
    )(
        *(
            pltpu.with_memory_space_constraint(array, pltpu.HBM)
            for array in (fluid_data, center_data, poly_coef.T)
        )
    )
    return pl.pallas_call(
        deliver,
        out_shape=shapes,
        in_specs=[vmem] * 2,
        out_specs=(hbm, hbm),
        scratch_shapes=[pltpu.SemaphoreType.DMA((2,))],
        compiler_params=pltpu.CompilerParams(vmem_limit_bytes=2**20),
        name="deliver",
    )(*outputs)


def solution(mesh):
    return jax.shard_map(
        per_device,
        mesh=mesh,
        in_specs=(P(None, ("row", "col")), P(None, ("col", "row")), P()),
        out_specs=(P(None, ("row", "col")), P(None, ("col", "row"))),
        check_vma=False,
    )
```
